32 devices in a mesh: groups: 2 (over x), ep: 8 (over z, y), section: 2 (over core).
Axes of the slice: x: 2, y: 2, z: 4, core: 2. Of those that a mesh axis runs over, the one named last changes fastest.
Arguments:
- resid: bfloat16 [2048, 4096], P(('groups', 'ep')), parts along dimension 0, may hold values from -6 to 6
- norm_gain: bfloat16 [4096], replicated, may hold values from 0.3984375 to 1.59375
- gate_logits: float32 [2048, 8], P(('groups', 'ep')), parts along dimension 0, may hold values from 0.1 to 1
- routes: int32 [2048, 8], P(('groups', 'ep')), parts along dimension 0, may hold values from 0 to 31, all different within a row; in each aligned block of 128 rows (0 to 127, 128 to 255, ...) at most 40 rows name the same one
- w_gate: bfloat16 [32, 4096, 768], P('ep', None, 'section'), may hold values from -0.09375 to 0.09375
- w_up: bfloat16 [32, 4096, 768], P('ep', None, 'section'), may hold values from -0.09375 to 0.09375
- w_down: bfloat16 [32, 768, 4096], P('ep', 'section'), may hold values from -0.21875 to 0.21875
- keys_raw: bfloat16 [2048, 512], P(('groups', 'ep'), 'section'), parts along dimension 0, may hold values from -6 to 6
- values_raw: bfloat16 [2048, 512], P(('groups', 'ep'), 'section'), parts along dimension 0, may hold values from -6 to 6
- k_gain: bfloat16 [128], replicated, may hold values from 0.25 to 1.75
- lengths: int32 [16], P(('groups', 'ep')), parts along dimension 0, may hold values from 32 to 128
- page_owner: int32 [16, 8], P(('groups', 'ep')), parts along dimension 0, may hold values from 0 to 7, as said below
- page_slot: int32 [16, 8], P(('groups', 'ep')), parts along dimension 0, may hold values from 0 to 7, as said below
Outputs:
- moe_out: bfloat16 [2048, 4096], P(('groups', 'ep'), 'section'), parts along dimension 0
- kv_cache: bfloat16 [128, 16, 2, 512], P(('groups', 'ep'), None, None, 'section'), parts along dimension 0
The draws below stay inside these ranges and needn't reach their ends.
There are 2 independent parts, one for each index of `groups`. The reference program is written for one: setup_inputs(seed, part) draws one part's arguments, and reference() takes and returns one part's arrays. A program takes and returns all parts, laid end to end along the dimension named above; an argument that names none is the same for every part. Nothing has to cross between parts.
Inputs may be any that keep to these rules, and one draw needn't show every extreme that they name: `page_owner`: each prompt sends its 8 pages to 4 different owners, exactly 2 pages to each of them; every owner receives exactly 8 pages. `page_slot`: the pages that reach one owner have different slots, so every slot of every owner is filled once.
All inputs are finite; a program needn't handle non-finite values.
Results may differ from the reference program's by a relative error of at most 0.0076.
Values may be sent and summed in bfloat16 or wider, within the bound.
A program may use at most 128 MiB of HBM per device.

```python
import math
import jax
import jax.numpy as jnp
import numpy as np
from jax import lax

D = 4096
HEAD = 128
KV_HEADS = 4
TOP = 8
FF = 768
EXPERTS = 32
TOK_DEV = 128
PAGE = 16
CAP = 40
PAGES = 8
SEQS = 8
TOKENS = 1024


def page_plan(key):
    base = jax.random.fold_in(key, 4242)
    streams = jax.random.split(base, 5)
    owner_order = jax.random.permutation(streams[0], SEQS)
    source_order = jax.random.permutation(streams[1], SEQS)
    shifts = jax.random.permutation(streams[2], SEQS)[:PAGES // 2]
    group_owner = owner_order[(source_order[:, None] + shifts[None, :]) % SEQS]
    column_perm = jax.vmap(lambda sub: jax.random.permutation(sub, PAGES))(jax.random.split(streams[3], SEQS))
    owner = jnp.take_along_axis(group_owner, column_perm // 2, axis=1)
    slot_perm = jax.vmap(lambda sub: jax.random.permutation(sub, PAGES))(jax.random.split(streams[4], SEQS))
    slot = slot_perm[owner, column_perm]
    return (owner.astype(jnp.int32), slot.astype(jnp.int32))


def draw_page_owner(key, part):
    return page_plan(key)[0]


def draw_page_slot(key, part):
    return page_plan(key)[1]


def plant(values, stream_key, least, largest):
    spot = [jax.random.randint(jax.random.fold_in(stream_key, axis), (), 0, length) for axis, length in enumerate(values.shape)]
    longest = values.shape.index(max(values.shape))
    beside = spot[:longest] + [(spot[longest] + 1) % values.shape[longest]] + spot[longest + 1:]
    return values.at[tuple(spot)].set(least).at[tuple(beside)].set(largest)


def level_of(key, shape, shards, low, top_value):
    def one(dim, parts):
        steps = jax.random.uniform(jax.random.fold_in(jax.random.fold_in(key, 6), dim), (parts,), jnp.float32, low / len(shards), top_value / len(shards))
        return jnp.repeat(jnp.exp(steps), shape[dim] // parts).reshape((-1,) + (1,) * (len(shape) - dim - 1))

    level = one(*shards[0])
    for cut in shards[1:]:
        level = level * one(*cut)
    return level


def deal_out(stream_key, own, number, rows, number_of, top, limit, slope):
    sequence = jax.random.permutation(stream_key, number_of)
    packed, ordinary = shares(number_of, rows * top, limit, slope, True), shares(number_of, rows * top, limit, slope, False)
    places = jnp.arange(number_of)

    def named(sizes, offset_by):
        used = int((sizes > 0).sum())
        fixed = max(1, used // 4)
        moved = fixed + (places - fixed + offset_by * (used - fixed)) % max(1, number_of - fixed)
        return jnp.zeros((number_of,), jnp.int32).at[sequence[jnp.where(places < fixed, places, moved)]].set(jnp.asarray(sizes, jnp.int32))

    sizes = jnp.where(number % 4 == 0, named(packed, number // 4), named(ordinary, number - number // 4 - 1))
    mixed = jax.random.permutation(jax.random.fold_in(own, 3), number_of)
    source_of, sink = mixed[0:number_of // 2 * 2:2], mixed[1:number_of // 2 * 2:2]
    room = jnp.minimum(sizes[source_of] - 1, limit - sizes[sink]) // 2
    room = jnp.where((source_of == sequence[0]) | (sink == sequence[0]) | (sizes[sink] == 0), 0, jnp.maximum(room, 0))
    moved = jax.random.randint(jax.random.fold_in(own, 4), (number_of // 2,), 0, 1 << 20) % (room + 1)
    sizes = sizes.at[source_of].add(-moved).at[sink].add(moved)
    labels = jnp.searchsorted(jnp.cumsum(sizes), jnp.arange(rows * top), side="right").astype(jnp.int32)
    listing = labels.reshape(top, rows).T
    listing = listing[jax.random.permutation(jax.random.fold_in(own, 1), rows)]
    offset_by = jax.random.randint(jax.random.fold_in(own, 2), (rows, 1), 0, top)
    return jnp.take_along_axis(listing, (jnp.arange(top)[None, :] + offset_by) % top, axis=1)


def shares(number_of, total, limit, skew, full):
    loads = [(1 << 20) // math.isqrt(grade ** skew) + 1 for grade in range(1, number_of + 1)]
    largest = limit if full else min(limit, max(-(-total // number_of), total * loads[0] // sum(loads)))
    least = 1 if total - largest >= number_of - 1 else 0
    holding, spare = [largest] + [least] * (number_of - 1), total - largest - least * (number_of - 1)
    while spare > 0:
        movable = [i for i in range(1, number_of) if holding[i] < largest] or [i for i in range(1, number_of) if holding[i] < limit]
        pool, budget = sum([loads[i] for i in movable]), spare
        for i in movable:
            more = min(limit - holding[i], max(1, budget * loads[i] // pool), spare)
            holding[i] = holding[i] + more
            spare = spare - more
    return np.array(holding)


def noise(stream_key, shape, spread, bound, shards=(), kind=jnp.bfloat16):
    array = spread * jax.random.normal(stream_key, shape, jnp.float32)
    if shards:
        array = array * level_of(stream_key, shape, shards, -0.22, 0.18)
    return jnp.clip(array, -bound, bound).astype(kind)


def setup_inputs(seed: int = 0, part: int = 0) -> dict:
    arg_keys = jax.random.split(jax.random.key(seed), 14)
    part_keys = jax.random.split(jax.random.fold_in(arg_keys[13], part), 14)
    resid = noise(part_keys[0], (TOKENS, D), 1.0, 6.0, ((0, 8),))
    norm_gain = jnp.clip(1.0 + 0.12 * jax.random.normal(arg_keys[1], (D,), jnp.float32), 0.3984375, 1.59375).astype(jnp.bfloat16)
    gate_logits = jnp.clip(jnp.exp(math.log(1.0) - 2.3025851 * jax.random.uniform(part_keys[2], (TOKENS, TOP), jnp.float32) ** level_of(part_keys[2], (TOKENS, TOP), ((0, 8),), -0.2, 0.2)), 0.1, 1.0)
    routes_keys = jax.random.split(jax.random.fold_in(part_keys[3], 1), TOKENS // TOK_DEV)
    routes_turns = jax.random.permutation(jax.random.fold_in(part_keys[3], 3), TOKENS // TOK_DEV)
    routes = jax.vmap(lambda own, number: deal_out(jax.random.fold_in(part_keys[3], 2), own, number, TOK_DEV, EXPERTS, TOP, CAP, 1))(routes_keys, routes_turns).reshape((TOKENS, TOP))
    w_gate = noise(arg_keys[4], (EXPERTS, D, FF), D ** -0.5, 0.09375, ((0, 8), (2, 2)))
    w_up = noise(arg_keys[5], (EXPERTS, D, FF), D ** -0.5, 0.09375, ((0, 8), (2, 2)))
    w_down = noise(arg_keys[6], (EXPERTS, FF, D), FF ** -0.5, 0.21875, ((0, 8), (1, 2)))
    keys_raw = noise(part_keys[7], (TOKENS, KV_HEADS * HEAD), 1.0, 6.0, ((0, 8), (1, 2)))
    values_raw = noise(part_keys[8], (TOKENS, KV_HEADS * HEAD), 1.0, 6.0, ((0, 8), (1, 2)))
    k_gain = jnp.clip(1.0 + 0.15 * jax.random.normal(arg_keys[9], (HEAD,), jnp.float32), 0.25, 1.75).astype(jnp.bfloat16)
    lengths = plant(jax.random.randint(part_keys[10], (SEQS,), TOK_DEV // 4, TOK_DEV + 1), jax.random.fold_in(part_keys[10], 1), TOK_DEV // 4, TOK_DEV).astype(jnp.int32)
    page_owner = draw_page_owner(jax.random.fold_in(jax.random.fold_in(arg_keys[13], part), 71), part)
    page_slot = draw_page_slot(jax.random.fold_in(jax.random.fold_in(arg_keys[13], part), 71), part)
    return {"resid": resid, "norm_gain": norm_gain, "gate_logits": gate_logits, "routes": routes, "w_gate": w_gate, "w_up": w_up, "w_down": w_down, "keys_raw": keys_raw, "values_raw": values_raw, "k_gain": k_gain, "lengths": lengths, "page_owner": page_owner, "page_slot": page_slot}


def rms_scale(values, gain_row):
    mean_square = lax.optimization_barrier(jnp.mean(values * values, axis=-1, keepdims=True))
    return values * lax.rsqrt(mean_square + 1e-06) * gain_row

def rotate_keys(key_block, position):
    half_size = key_block.shape[-1] // 2
    frequency = jnp.exp(jnp.arange(half_size, dtype=jnp.float32) * (-2.0 / key_block.shape[-1]) * math.log(1000000.0))
    angles = position.astype(jnp.float32)[:, None, None] * frequency
    cosine = jnp.cos(angles)
    sine_part = jnp.sin(angles)
    first_half = key_block[..., :half_size]
    second = key_block[..., half_size:]
    return jnp.concatenate([first_half * cosine - second * sine_part, second * cosine + first_half * sine_part], axis=-1)

def reference(resid, norm_gain, gate_logits, routes, w_gate, w_up, w_down, keys_raw, values_raw, k_gain, lengths, page_owner, page_slot):
    total_tokens = SEQS * TOK_DEV
    token_ids = jnp.arange(total_tokens, dtype=jnp.int32)
    position = token_ids % TOK_DEV
    prompt_ids = token_ids // TOK_DEV
    is_live = position < lengths[prompt_ids]
    hidden = rms_scale(resid.astype(jnp.float32), norm_gain.astype(jnp.float32)).astype(jnp.bfloat16)
    logits = gate_logits.astype(jnp.float32)
    mixing = (logits / lax.optimization_barrier(jnp.sum(logits, axis=-1, keepdims=True))).astype(jnp.bfloat16)
    pair_count = TOK_DEV * TOP
    chosen = routes.reshape(SEQS, pair_count).astype(jnp.int32)
    live_rows = jnp.repeat(is_live, TOP).reshape(SEQS, pair_count)
    expert_hits = ((chosen[:, :, None] == jnp.arange(EXPERTS, dtype=jnp.int32)[None, None, :]) & live_rows[:, :, None]).astype(jnp.int32)
    slot_rank = lax.optimization_barrier(jnp.sum((jnp.cumsum(expert_hits, axis=1) - expert_hits) * expert_hits, axis=2))
    slot_span = SEQS * CAP
    dead_slot = EXPERTS * slot_span
    target = jnp.where(live_rows, chosen * slot_span + jnp.arange(SEQS, dtype=jnp.int32)[:, None] * CAP + slot_rank, dead_slot).astype(jnp.int32)
    row_token = jnp.repeat(token_ids, TOP).reshape(SEQS, pair_count)
    table = jnp.full((dead_slot + 1,), total_tokens, jnp.int32).at[target.reshape(-1)].set(row_token.reshape(-1))
    table = table[:dead_slot].reshape(EXPERTS, slot_span)
    padded = jnp.concatenate([hidden, jnp.zeros((1, D), jnp.bfloat16)], axis=0)

    def one_expert(expert_index):
        gathered = padded[table[expert_index]]
        gate_part = jnp.dot(gathered, w_gate[expert_index], preferred_element_type=jnp.float32)
        up_part = jnp.dot(gathered, w_up[expert_index], preferred_element_type=jnp.float32)
        active = (jax.nn.silu(gate_part) * up_part).astype(jnp.bfloat16)
        return jnp.dot(active, w_down[expert_index], preferred_element_type=jnp.float32).astype(jnp.bfloat16)
    expert_out = lax.map(one_expert, jnp.arange(EXPERTS, dtype=jnp.int32))
    flat_out = jnp.concatenate([expert_out.reshape(dead_slot, D), jnp.zeros((1, D), jnp.bfloat16)], axis=0)
    pair_slot = target.reshape(total_tokens, TOP)
    mixed = jnp.zeros((total_tokens, D), jnp.float32)
    for pick_index in range(TOP):
        mixed = mixed + mixing[:, pick_index].astype(jnp.float32)[:, None] * flat_out[pair_slot[:, pick_index]].astype(jnp.float32)
    moe_out = mixed.astype(jnp.bfloat16)
    head_rows = keys_raw.astype(jnp.float32).reshape(total_tokens, KV_HEADS, HEAD)
    normed = rms_scale(head_rows, k_gain.astype(jnp.float32))
    turned = rotate_keys(normed, position)
    key_rows = jnp.where(is_live[:, None, None], turned, 0.0).astype(jnp.bfloat16).reshape(total_tokens, KV_HEADS * HEAD)
    value_rows = jnp.where(is_live[:, None], values_raw, jnp.zeros_like(values_raw))
    stacked = jnp.stack([key_rows, value_rows], axis=1).reshape(SEQS * PAGES, PAGE, 2, KV_HEADS * HEAD)
    destination = (page_owner.astype(jnp.int32) * PAGES + page_slot.astype(jnp.int32)).reshape(-1)
    kv_cache = jnp.zeros_like(stacked).at[destination].set(stacked)
    return (moe_out, kv_cache)
```

```python
import functools
import math

import jax
import jax.numpy as jnp
from jax import lax
from jax.experimental import pallas as pl
from jax.experimental.pallas import tpu as pltpu
from jax.sharding import PartitionSpec as P

PAGE = 16
CAP = 40
F32 = jnp.float32
BF16 = jnp.bfloat16


def rms_scale(values, gain_row):
    mean_square = jnp.mean(values * values, axis=-1, keepdims=True)
    return values * lax.rsqrt(mean_square + 1e-06) * gain_row


def rotate_keys(key_block, position):
    half_size = key_block.shape[-1] // 2
    frequency = jnp.exp(
        jnp.arange(half_size, dtype=F32) * (-2.0 / key_block.shape[-1]) * math.log(1000000.0)
    )
    angles = position.astype(F32)[:, None, None] * frequency
    cosine = jnp.cos(angles)
    sine_part = jnp.sin(angles)
    first_half = key_block[..., :half_size]
    second = key_block[..., half_size:]
    return jnp.concatenate(
        [first_half * cosine - second * sine_part, second * cosine + first_half * sine_part],
        axis=-1,
    )


MESH = pl.DeviceIdType.MESH


def greet(outer, inner, z, y, ep, core, halves):
    barrier = pltpu.get_barrier_semaphore()

    def signal(to_ep, to_core):
        pl.semaphore_signal(
            barrier, inc=1, device_id={"ep": to_ep, "section": to_core}, device_id_type=MESH
        )

    pl.when(z > 0)(lambda: signal(ep - inner, core))
    pl.when(z < outer - 1)(lambda: signal(ep + inner, core))
    for k in range(1, inner):
        signal(z * inner + lax.rem(y + k, inner), core)
    for k in range(1, halves):
        signal(ep, lax.rem(core + k, halves))
    ends = jnp.where(z > 0, 1, 0) + jnp.where(z < outer - 1, 1, 0)
    pl.semaphore_wait(barrier, ends + inner - 1 + halves - 1)


def place(outer, inner):
    ep = lax.axis_index("ep")
    return ep, lax.axis_index("section"), lax.div(ep, inner), lax.rem(ep, inner)


def columns(ref, block, half, cols):
    return ref.at[block, :, pl.ds(pl.multiple_of(half * cols, cols), cols)]


def by_distance(outer, z, order, body):
    for d in order:
        for side in (-1, 1) if d else (1,):
            zz = z + side * d
            if d:
                pl.when((zz >= 0) & (zz < outer))(functools.partial(body, d, side, zz))
            else:
                body(d, side, zz)


def gather_kernel(outer, inner, halves, src, meta, out, mout, send, recv, msend, mrecv, local):
    ep, core, z, y = place(outer, inner)
    cols = src.shape[1]
    own = pltpu.make_async_copy(src, columns(out, ep, core, cols), local.at[0])
    mown = pltpu.make_async_copy(meta, mout.at[ep], local.at[1])
    own.start()
    mown.start()
    greet(outer, inner, z, y, ep, core, halves)
    own.wait()
    mown.wait()
    to_sibling = 1 + inner

    def rows_copy(block, half, kind, to_ep, to_core):
        return pltpu.make_async_remote_copy(
            src_ref=columns(out, block, half, cols),
            dst_ref=columns(out, block, half, cols),
            send_sem=send.at[kind, block],
            recv_sem=recv.at[block, half],
            device_id={"ep": to_ep, "section": to_core},
            device_id_type=MESH,
        )

    def meta_copy(block, kind, to_ep):
        return pltpu.make_async_remote_copy(
            src_ref=mout.at[block],
            dst_ref=mout.at[block],
            send_sem=msend.at[kind, block],
            recv_sem=mrecv.at[block],
            device_id={"ep": to_ep, "section": core},
            device_id_type=MESH,
        )

    def chip_copies(block, kind, to_ep, act):
        act(meta_copy(block, kind, to_ep))
        act(rows_copy(block, core, kind, to_ep, core))

    def column(block, d, side, act):
        if d == 0 or side == 1:
            pl.when(z > 0)(lambda: chip_copies(block, 0, ep - inner, act))
        if d == 0 or side == -1:
            pl.when(z < outer - 1)(lambda: chip_copies(block, 1, ep + inner, act))
        for k in range(1, inner):
            chip_copies(block, 1 + k, z * inner + lax.rem(y + k, inner), act)

    def sibling(block, act):
        for k in range(1, halves):
            act(rows_copy(block, core, to_sibling + k - 1, ep, lax.rem(core + k, halves)))

    def start(copy):
        copy.start()

    def wait_send(copy):
        copy.wait_send()

    def arrived(block, half):
        rows_copy(block, half, 0, ep, core).wait_recv()

    def step(d, side, zz):
        block = zz * inner + y
        if d:
            meta_copy(block, 0, ep).wait_recv()
            arrived(block, core)
        column(block, d, side, start)
        sibling(block, start)

    def across(d, side, zz):
        for k in range(1, inner):
            block = zz * inner + lax.rem(y + k, inner)
            meta_copy(block, 0, ep).wait_recv()
            arrived(block, core)
            sibling(block, start)

    def finish(d, side, zz):
        column(zz * inner + y, d, side, wait_send)
        for yy in range(inner):
            block = zz * inner + yy
            sibling(block, wait_send)
            for k in range(1, halves):
                arrived(block, lax.rem(core + k, halves))

    for d in range(outer + 1):
        if d < outer:
            by_distance(outer, z, (d,), step)
        if d > 0:
            by_distance(outer, z, (d - 1,), across)
    by_distance(outer, z, range(outer), finish)


def gather_rows(outer, inner, halves, hidden, meta):
    peers = outer * inner
    kinds = 1 + inner + halves - 1
    dma = pltpu.SemaphoreType.DMA
    vmem = pl.BlockSpec(memory_space=pltpu.VMEM)
    return pl.pallas_call(
        functools.partial(gather_kernel, outer, inner, halves),
        out_shape=(
            jax.ShapeDtypeStruct((peers, hidden.shape[0], halves * hidden.shape[1]), hidden.dtype),
            jax.ShapeDtypeStruct((peers,) + meta.shape, meta.dtype),
        ),
        in_specs=[vmem, vmem],
        out_specs=(vmem, vmem),
        scratch_shapes=[
            dma((kinds, peers)),
            dma((peers, halves)),
            dma((kinds, peers)),
            dma((peers,)),
            dma((2,)),
        ],
        compiler_params=pltpu.CompilerParams(collective_id=0, has_side_effects=True),
        name="gather_rows",
    )(hidden, meta)


def scatter_kernel(
    outer, inner, halves, mixed, out, acc, sib, yb, zb, lsem, ssend, srecv, ysend, yrecv, zsend, zrecv
):
    ep, core, z, y = place(outer, inner)
    other = halves - 1 - core
    tok, cols = out.shape

    def local_copy(block):
        return pltpu.make_async_copy(
            columns(mixed, block, core, cols), acc.at[block], lsem.at[block]
        )

    def sib_copy(block):
        return pltpu.make_async_remote_copy(
            src_ref=columns(mixed, block, other, cols),
            dst_ref=sib.at[block],
            send_sem=ssend.at[block],
            recv_sem=srecv.at[block],
            device_id={"ep": ep, "section": other},
            device_id_type=MESH,
        )

    def y_copy(zz, k):
        to_y = lax.rem(y + k, inner)
        return pltpu.make_async_remote_copy(
            src_ref=acc.at[zz * inner + to_y],
            dst_ref=yb.at[k - 1, zz],
            send_sem=ysend.at[k - 1, zz],
            recv_sem=yrecv.at[k - 1, zz],
            device_id={"ep": z * inner + to_y, "section": core},
            device_id_type=MESH,
        )

    def z_copy(zz, slot, to_ep):
        return pltpu.make_async_remote_copy(
            src_ref=acc.at[zz * inner + y],
            dst_ref=zb.at[slot],
            send_sem=zsend.at[zz],
            recv_sem=zrecv.at[slot],
            device_id={"ep": to_ep, "section": core},
            device_id_type=MESH,
        )

    def add(dst, *sources):
        def body(i, carry):
            piece = pl.ds(pl.multiple_of(i * 16, 16), 16)
            total = sources[0][piece, :].astype(F32)
            for source in sources[1:]:
                total = total + source[piece, :].astype(F32)
            dst[piece, :] = total.astype(dst.dtype)
            return carry

        lax.fori_loop(0, tok // 16, body, 0)

    greet(outer, inner, z, y, ep, core, halves)
    far_first = range(outer - 1, -1, -1)

    def open_step(d, side, zz):
        for k in list(range(1, inner)) + [0]:
            block = zz * inner + lax.rem(y + k, inner)
            sib_copy(block).start()
            local_copy(block).start()

    def y_step(d, side, zz):
        for k in range(1, inner):
            block = zz * inner + lax.rem(y + k, inner)
            local_copy(block).wait()
            sib_copy(block).wait_recv()
            add(acc.at[block], acc.at[block], sib.at[block])
            y_copy(zz, k).start()

    def z_step(d, side, zz):
        block = zz * inner + y
        local_copy(block).wait()
        sib_copy(block).wait_recv()
        for k in range(1, inner):
            y_copy(zz, k).wait_recv()
        parts = [acc.at[block], sib.at[block]] + [yb.at[k, zz] for k in range(inner - 1)]
        target = acc.at[block] if d else out
        if d:
            feeds = (z - side >= 0) & (z - side < outer)
            slot = outer if (d == 1 and side == -1) else zz

            @pl.when(feeds)
            def _():
                z_copy(zz, zz, ep).wait_recv()
                add(target, *parts, zb.at[zz])

            @pl.when(jnp.logical_not(feeds))
            def _():
                add(target, *parts)

            z_copy(zz, slot, ep + side * inner).start()
            return

        @pl.when(z > 0)
        def _():
            z_copy(zz, zz, ep).wait_recv()

        @pl.when(z == 0)
        def _():
            z_copy(zz, outer, ep).wait_recv()
            add(out, *parts, zb.at[outer])

        @pl.when(z == outer - 1)
        def _():
            add(out, *parts, zb.at[zz])

        @pl.when((z > 0) & (z < outer - 1))
        def _():
            z_copy(zz, outer, ep).wait_recv()
            add(out, *parts, zb.at[zz], zb.at[outer])

    def close_step(d, side, zz):
        for k in range(inner):
            sib_copy(zz * inner + lax.rem(y + k, inner)).wait_send()
        for k in range(1, inner):
            y_copy(zz, k).wait_send()
        if d:
            z_copy(zz, zz, ep).wait_send()

    by_distance(outer, z, far_first, open_step)
    by_distance(outer, z, far_first, y_step)
    by_distance(outer, z, far_first, z_step)
    by_distance(outer, z, far_first, close_step)


def scatter_sums(outer, inner, halves, mixed):
    peers = outer * inner
    shape = (mixed.shape[1], mixed.shape[2] // halves)
    dma = pltpu.SemaphoreType.DMA
    across = max(inner - 1, 1)
    return pl.pallas_call(
        functools.partial(scatter_kernel, outer, inner, halves),
        out_shape=jax.ShapeDtypeStruct(shape, mixed.dtype),
        in_specs=[pl.BlockSpec(memory_space=pl.ANY)],
        out_specs=pl.BlockSpec(memory_space=pltpu.VMEM),
        scratch_shapes=[
            pltpu.VMEM((peers,) + shape, mixed.dtype),
            pltpu.VMEM((peers,) + shape, mixed.dtype),
            pltpu.VMEM((across, outer if inner > 1 else 1) + shape, mixed.dtype),
            pltpu.VMEM((outer + 1,) + shape, mixed.dtype),
            dma((peers,)),
            dma((peers,)),
            dma((peers,)),
            dma((across, outer)),
            dma((across, outer)),
            dma((outer,)),
            dma((outer + 1,)),
        ],
        compiler_params=pltpu.CompilerParams(collective_id=1, has_side_effects=True),
        name="scatter_sums",
    )(mixed)


def inner_size(mesh):
    try:
        line = mesh.devices[0, :, 0]
        coords = [tuple(device.coords) for device in line]
        inner = 1
        while inner < len(coords) and sum(a != b for a, b in zip(coords[inner], coords[0])) == 1:
            axis = [i for i in range(3) if coords[1][i] != coords[0][i]][0]
            if coords[inner][axis] == coords[0][axis]:
                break
            inner += 1
        return inner if inner < len(coords) and len(coords) % inner == 0 else 1
    except (AttributeError, IndexError, TypeError):
        return 1


def shards(
    inner,
    resid,
    norm_gain,
    gate_logits,
    routes,
    w_gate,
    w_up,
    w_down,
    keys_raw,
    values_raw,
    k_gain,
    lengths,
    page_owner,
    page_slot,
):
    tok_rows, model_width = resid.shape
    halves = lax.axis_size("section")
    peers = lax.axis_size("ep")
    me = lax.axis_index("ep")
    core = lax.axis_index("section")
    local_experts, _, ff_half = w_gate.shape
    experts = local_experts * peers
    cols = model_width // halves
    position = jnp.arange(tok_rows, dtype=jnp.int32)
    is_live = position < lengths[0]

    wide = resid.astype(F32)
    scale = lax.rsqrt(jnp.mean(wide * wide, axis=-1, keepdims=True) + 1e-06)
    my_cols = lax.dynamic_slice_in_dim(resid, core * cols, cols, 1).astype(F32)
    my_gain = lax.dynamic_slice_in_dim(norm_gain, core * cols, cols, 0).astype(F32)
    hidden = (my_cols * scale * my_gain).astype(BF16)
    mixing = (gate_logits / jnp.sum(gate_logits, axis=-1, keepdims=True)).astype(BF16)
    expert_ids = jnp.arange(experts, dtype=jnp.int32)
    named = (routes[:, :, None] == expert_ids) & is_live[:, None, None]
    hits = jnp.any(named, axis=1)
    weight = jnp.sum(jnp.where(named, mixing.astype(F32)[:, :, None], 0.0), axis=1)
    earlier = (position[:, None] > position[None, :]).astype(BF16)
    rank = jnp.dot(earlier, hits.astype(BF16), preferred_element_type=F32)
    rank = jnp.where(hits, rank, -1.0)
    page_to = (page_owner * page_owner.shape[1] + page_slot).astype(F32)
    page_to = jnp.broadcast_to(page_to, (tok_rows, page_to.shape[1]))
    small = jnp.concatenate([rank, weight, page_to], axis=1).astype(BF16)
    small = jnp.pad(small, ((0, 0), (0, -small.shape[1] % 128)))
    rows, small = gather_rows(peers // inner, inner, halves, hidden, small)
    small = small.astype(F32)
    first = me * local_experts
    rank_in = lax.dynamic_slice_in_dim(small, first, local_experts, 2)
    weight_in = lax.dynamic_slice_in_dim(small, experts + first, local_experts, 2)
    page_in = small[:, 0, 2 * experts : 2 * experts + page_owner.shape[1]].reshape(-1)

    head = k_gain.shape[0]
    heads_local = keys_raw.shape[1] // head
    kv_width = keys_raw.shape[1]
    normed = rms_scale(
        keys_raw.astype(F32).reshape(tok_rows, heads_local, head), k_gain.astype(F32)
    )
    turned = rotate_keys(normed, position)
    key_rows = (
        jnp.where(is_live[:, None, None], turned, 0.0).astype(BF16).reshape(tok_rows, kv_width)
    )
    value_rows = jnp.where(is_live[:, None], values_raw, jnp.zeros_like(values_raw))
    pages = page_owner.shape[1]
    page_rows = jnp.stack([key_rows, value_rows], axis=1).reshape(pages, PAGE * 2 * kv_width)
    all_pages = lax.all_gather(page_rows, "ep", axis=0, tiled=True)
    slots = me * pages + jnp.arange(pages, dtype=jnp.int32)
    choose = (slots.astype(F32)[:, None] == page_in[None, :]).astype(BF16)
    kv_cache = jnp.dot(choose, all_pages, preferred_element_type=F32).astype(BF16)
    kv_cache = kv_cache.reshape(pages, PAGE, 2, kv_width)

    slot_ids = jnp.arange(CAP, dtype=jnp.int32).astype(F32)
    dispatch = (
        jnp.swapaxes(rank_in, 1, 2)[:, :, None, :] == slot_ids[:, None]
    ).astype(BF16)
    dispatch = dispatch.reshape(peers, local_experts * CAP, tok_rows)
    combine = jnp.where(rank_in[..., None] == slot_ids, weight_in[..., None], 0.0).astype(BF16)
    combine = combine.reshape(peers, tok_rows, local_experts * CAP)
    arrived = jnp.einsum("sct,std->scd", dispatch, rows, preferred_element_type=F32)
    arrived = arrived.astype(BF16).reshape(peers, local_experts, CAP, halves * cols)
    gate_part = jnp.einsum("sjcd,jdf->sjcf", arrived, w_gate, preferred_element_type=F32)
    up_part = jnp.einsum("sjcd,jdf->sjcf", arrived, w_up, preferred_element_type=F32)
    active = (jax.nn.silu(gate_part) * up_part).astype(BF16)
    part = jnp.einsum("sjcf,jfd->sjcd", active, w_down, preferred_element_type=F32).astype(BF16)
    part = part.reshape(peers, local_experts * CAP, model_width)
    mixed = jnp.einsum("stc,scd->std", combine, part, preferred_element_type=F32).astype(BF16)
    moe_out = scatter_sums(peers // inner, inner, halves, mixed)
    return (moe_out, kv_cache)


def solution(mesh):
    in_specs = (
        P(("groups", "ep"), None),
        P(),
        P(("groups", "ep"), None),
        P(("groups", "ep"), None),
        P("ep", None, "section"),
        P("ep", None, "section"),
        P("ep", "section", None),
        P(("groups", "ep"), "section"),
        P(("groups", "ep"), "section"),
        P(),
        P(("groups", "ep")),
        P(("groups", "ep"), None),
        P(("groups", "ep"), None),
    )
    out_specs = (P(("groups", "ep"), "section"), P(("groups", "ep"), None, None, "section"))
    body = functools.partial(shards, inner_size(mesh))
    return jax.shard_map(body, mesh=mesh, in_specs=in_specs, out_specs=out_specs, check_vma=False)
```
